32 devices in a mesh: groups: 2 (over y), seq: 8 (over z, x), sub: 2 (over core).
Axes of the slice: x: 2, y: 2, z: 4, core: 2. Of those that a mesh axis runs over, the one named last changes fastest.
Arguments:
- cache_in: bfloat16 [64, 2, 36864], P('groups', None, ('sub', 'seq')), parts along dimension 0, may hold values from -6 to 6
- page_counts: int32 [16], P('groups'), parts along dimension 0, may hold values from 1 to 8, 32 in all
- tail_tokens: int32 [16], P('groups'), parts along dimension 0, may hold values from 1 to 64
- assignment: int32 [16], P('groups'), parts along dimension 0, may hold values from 0 to 7, each once
Outputs:
- cache_out: bfloat16 [128, 2, 36864], P(('groups', 'seq'), None, 'sub'), parts along dimension 0
- checksum: float32 [2, 128], P(None, ('groups', 'seq')), parts along dimension 1
The draws below stay inside these ranges and needn't reach their ends.
There are 2 independent parts, one for each index of `groups`. The reference program is written for one: setup_inputs(seed, part) draws one part's arguments, and reference() takes and returns one part's arrays. A program takes and returns all parts, laid end to end along the dimension named above; each array names one. Nothing has to cross between parts.
Inputs may be any that keep to these rules, and one draw needn't show every extreme that they name: `page_counts`: the page counts sum to 32. `assignment`: every seq index serves exactly one request.
All inputs are finite; a program needn't handle non-finite values.
Results may differ from the reference program's by a relative error of at most 0.001.
Values may be sent and summed in bfloat16 or wider, within the bound.
A program may use at most 64 MiB of HBM per device.

```python
import math
import jax
import jax.numpy as jnp
import numpy as np
from jax import lax

LATENT = 576
PAGE = 64
LAYERS = 2
MAXP = 8
REQS = 8
PAGES = 32
SLOTS = 64
ROW = 36864
N_SEQ = 8


def touch_ends(entries, rng, smallest, largest):
    spot = [jax.random.randint(jax.random.fold_in(rng, axis), (), 0, length) for axis, length in enumerate(entries.shape)]
    longest = entries.shape.index(max(entries.shape))
    beside = spot[:longest] + [(spot[longest] + 1) % entries.shape[longest]] + spot[longest + 1:]
    return entries.at[tuple(spot)].set(smallest).at[tuple(beside)].set(largest)


def steps_of(rng, dims, pieces, smallest, high):
    def one(axis_at, blocks):
        draws = jax.random.uniform(jax.random.fold_in(jax.random.fold_in(rng, 6), axis_at), (blocks,), jnp.float32, smallest / len(pieces), high / len(pieces))
        return jnp.repeat(jnp.exp(draws), dims[axis_at] // blocks).reshape((-1,) + (1,) * (len(dims) - axis_at - 1))

    level = one(*pieces[0])
    for cut in pieces[1:]:
        level = level * one(*cut)
    return level


def profile(amount, total, bound, skew):
    weights = [(1 << 20) // math.isqrt(standing ** skew) + 1 for standing in range(2, amount + 1)]
    spare, counts = total - bound - (amount - 1), [1] * (amount - 1)
    while spare > 0:
        free = [i for i in range(amount - 1) if counts[i] < bound]
        mass, budget = sum([weights[i] for i in free]), spare
        for i in free:
            extra = min(bound - counts[i], max(1, budget * weights[i] // mass), spare)
            counts[i] = counts[i] + extra
            spare = spare - extra
    return np.array([bound] + counts)


def ragged_sizes(key, amount, total, reach, slope):
    if amount == 2:
        one = jax.random.randint(key, (), max(1, total - reach), min(reach, total - 1) + 1)
        return jnp.stack([one, total - one])
    sizes = jnp.asarray(profile(amount, total, reach, slope), jnp.int32)
    pairs = (amount - 1) // 2
    giver, receiver = sizes[1:1 + 2 * pairs:2], sizes[2:2 + 2 * pairs:2]
    margin = jnp.minimum(giver - 1, reach - receiver)
    passed = jax.random.randint(jax.random.fold_in(key, 1), (pairs,), 0, 1 << 20) % (margin + 1)
    sizes = sizes.at[1:1 + 2 * pairs:2].set(giver - passed).at[2:2 + 2 * pairs:2].set(receiver + passed)
    return sizes[jax.random.permutation(jax.random.fold_in(key, 2), amount)]


def scatter_about(key, dims, deviation, most, cuts=(), kind=jnp.bfloat16):
    drawn = deviation * jax.random.normal(key, dims, jnp.float32)
    if cuts:
        drawn = drawn * steps_of(key, dims, cuts, -0.22, 0.18)
    return jnp.clip(drawn, -most, most).astype(kind)


def setup_inputs(seed: int = 0, part: int = 0) -> dict:
    arg_keys = jax.random.split(jax.random.key(seed), 5)
    own_keys = jax.random.split(jax.random.fold_in(arg_keys[4], part), 5)
    return {
        "cache_in": scatter_about(own_keys[0], (PAGES, LAYERS, ROW), 1.0, 6.0, ((2, 16),)),
        "page_counts": ragged_sizes(own_keys[1], REQS, PAGES, MAXP, 2).astype(jnp.int32),
        "tail_tokens": touch_ends(jax.random.randint(own_keys[2], (REQS,), 1, PAGE + 1), jax.random.fold_in(own_keys[2], 1), 1, PAGE).astype(jnp.int32),
        "assignment": jax.random.permutation(own_keys[3], REQS).astype(jnp.int32),
    }


def reference(cache_in, page_counts, tail_tokens, assignment):
    starts = (jnp.cumsum(page_counts) - page_counts).astype(jnp.int32)
    request_ids = jnp.arange(REQS, dtype=jnp.int32)
    owners = jnp.zeros((REQS,), jnp.int32).at[assignment].set(request_ids)
    page_ids = jnp.arange(MAXP, dtype=jnp.int32)
    token_of = jnp.arange(ROW, dtype=jnp.int32) // LATENT

    def one_device(device):
        request = owners[device]
        count = page_counts[request]
        begin = starts[request]
        tail = tail_tokens[request]
        in_use = page_ids < count
        source_rows = jnp.where(in_use, begin + page_ids, 0).astype(jnp.int32)
        filled = jnp.where(in_use, jnp.where(page_ids < count - 1, PAGE, tail), 0)
        fetched = jnp.take(cache_in, source_rows, axis=0)
        kept_mask = token_of[None, :] < filled[:, None]
        fetched = jnp.where(kept_mask[:, None, :], fetched, jnp.zeros((), cache_in.dtype))
        squares = lax.optimization_barrier(jnp.sum(jnp.square(fetched.astype(jnp.float32)), axis=2))
        return (fetched, squares)
    pages_all, squares_all = lax.map(one_device, jnp.arange(N_SEQ, dtype=jnp.int32))
    cache_out = pages_all.reshape(SLOTS, LAYERS, ROW)
    squares_all = squares_all.reshape(SLOTS, LAYERS)
    checksum = jnp.sqrt(1.0 + squares_all / ROW).T
    return (cache_out, checksum)
```

```python
import functools

import jax
import jax.numpy as jnp
from jax import lax
from jax.experimental import pallas as pl
from jax.experimental.pallas import tpu as pltpu
from jax.sharding import PartitionSpec as P

LATENT = 576
PAGE = 64
MAXP = 8
LANES = 128
MESH = pl.DeviceIdType.MESH


def by_device(matches, values):
    return jnp.sum(jnp.where(matches, values[None, :], 0), axis=1)


def general(cache_in, page_counts, tail_tokens, assignment):
    seq_count = lax.axis_size("seq")
    own_index = lax.axis_index("seq")
    sub_index = lax.axis_index("sub")
    total_pages, layer_count, piece = cache_in.shape
    starts = jnp.cumsum(page_counts) - page_counts
    device_ids = jnp.arange(seq_count, dtype=jnp.int32)
    matches = assignment[None, :] == device_ids[:, None]
    dest_counts = by_device(matches, page_counts)
    dest_starts = by_device(matches, starts)
    dest_tails = by_device(matches, tail_tokens)
    slot_ids = jnp.arange(seq_count * MAXP, dtype=jnp.int32)
    page_rank = slot_ids % MAXP
    counts_at = jnp.repeat(dest_counts, MAXP)
    starts_at = jnp.repeat(dest_starts, MAXP)
    tails_at = jnp.repeat(dest_tails, MAXP)
    in_use = page_rank < counts_at
    source_rows = jnp.where(in_use, starts_at + page_rank, 0)
    filled = jnp.where(in_use, jnp.where(page_rank < counts_at - 1, PAGE, tails_at), 0)
    column = (sub_index * seq_count + own_index) * piece + jnp.arange(piece, dtype=jnp.int32)
    token_of = column // LATENT
    kept_mask = token_of[None, :] < filled[:, None]
    zero_value = jnp.zeros((), cache_in.dtype)
    fetched = jnp.take(cache_in, source_rows, axis=0)
    packed = jnp.where(kept_mask[:, None, :], fetched, zero_value)
    cache_out = lax.all_to_all(packed, "seq", split_axis=0, concat_axis=2, tiled=True)
    squares = jnp.sum(jnp.square(cache_out.astype(jnp.float32)), axis=2)
    squares = lax.psum(squares, "sub")
    checksum = jnp.sqrt(1.0 + squares / (PAGE * LATENT)).T
    return (cache_out, checksum)


def far_first(n):
    return sorted(range(1, n), key=lambda i: -min(i, n - i))


def exchange(n, subs, counts, tails, assign, x, out, chk, send, tab, part, parts_in,
             send_sem, recv_sem, psend_sem, precv_sem, own_sem):
    me = lax.axis_index("seq")
    sub = lax.axis_index("sub")
    pages, layers, piece = x.shape
    tokens = piece // LATENT
    own_id = me * subs + sub

    barrier = pltpu.get_barrier_semaphore()
    for i in range(n):
        for j in range(subs):
            if i or j:
                pl.semaphore_signal(
                    barrier, inc=1,
                    device_id={"seq": lax.rem(me + i, n), "sub": lax.rem(sub + j, subs)},
                    device_id_type=MESH)

    column = lax.broadcasted_iota(jnp.int32, (layers, piece), 1)
    for f in range(tokens + 1):
        tab[f] = jnp.where(column < f * LATENT, 1.0, 0.0).astype(x.dtype)

    reqs = counts.shape[0]
    packed, begin = [], jnp.int32(0)
    for r in range(reqs):
        packed.append((begin * 16 + counts[r]) * 128 + tails[r])
        begin = begin + counts[r]
    base = (sub * n + me) * tokens

    def gather(i):
        dest = lax.rem(me + i, n)
        info = jnp.int32(0)
        for r in range(reqs):
            info = info + jnp.where(assign[r] == dest, packed[r], 0)
        tail = info & 127
        count = (info >> 7) & 15
        start = info >> 11
        for k in range(MAXP):
            used = k < count
            row = jnp.where(used, start + k, 0)
            filled = jnp.where(used, jnp.where(k < count - 1, PAGE, tail), 0)
            keep = jnp.clip(filled - base, 0, tokens)
            send[i, k] = x[row] * tab[keep]

    def piece_copy(i):
        return pltpu.make_async_remote_copy(
            src_ref=send.at[i],
            dst_ref=out.at[:, :, pl.ds(pl.multiple_of(me * piece, LANES), piece)],
            send_sem=send_sem.at[i],
            recv_sem=recv_sem.at[me],
            device_id={"seq": lax.rem(me + i, n)},
            device_id_type=MESH)

    def part_copy(i, j):
        return pltpu.make_async_remote_copy(
            src_ref=part.at[i],
            dst_ref=parts_in.at[own_id],
            send_sem=psend_sem.at[i * subs + j],
            recv_sem=precv_sem.at[own_id],
            device_id={"seq": lax.rem(me + i, n), "sub": lax.rem(sub + j, subs)},
            device_id_type=MESH)

    order = far_first(n)
    gather(order[0])
    gather(order[1])
    pl.semaphore_wait(barrier, n * subs - 1)
    started = []
    for p, i in enumerate(order):
        if p >= 2:
            gather(i)
        if p >= 1:
            piece_copy(order[p - 1]).start()
    gather(0)
    piece_copy(order[-1]).start()

    lane = lax.broadcasted_iota(jnp.int32, (layers, LANES), 1)
    own_copy = pltpu.make_async_copy(
        send.at[0], out.at[:, :, pl.ds(pl.multiple_of(me * piece, LANES), piece)], own_sem)

    def squares(i):
        total = jnp.zeros((layers, LANES), jnp.float32)
        for k in range(MAXP):
            v = send[i, k].astype(jnp.float32)
            s = jnp.sum(v * v, axis=1, keepdims=True)
            total = jnp.where(lane == k, s, total)
        return total

    last = None
    for i in order:
        part[i] = squares(i)
        if last is None:
            own_copy.start()
        else:
            for j in range(subs):
                part_copy(last, j).start()
        last = i
    own = squares(0)
    part[0] = own
    for j in range(subs):
        part_copy(last, j).start()
    parts_in[own_id] = own
    for j in range(1, subs):
        part_copy(0, j).start()

    for i in range(n):
        for j in range(subs):
            if i or j:
                src = lax.rem(me + n - i, n) * subs + lax.rem(sub + j, subs)
                pltpu.make_async_remote_copy(
                    src_ref=part.at[i],
                    dst_ref=parts_in.at[src],
                    send_sem=psend_sem.at[i * subs + j],
                    recv_sem=precv_sem.at[src],
                    device_id={"seq": lax.rem(me + i, n), "sub": lax.rem(sub + j, subs)},
                    device_id_type=MESH).wait()
    total = jnp.sum(parts_in[...], axis=0)
    chk[...] = jnp.sqrt(1.0 + total / (PAGE * LATENT))[:, :MAXP]
    own_copy.wait()
    for i in order:
        src = lax.rem(me + n - i, n)
        pltpu.make_async_remote_copy(
            src_ref=send.at[i],
            dst_ref=out.at[:, :, pl.ds(pl.multiple_of(src * piece, LANES), piece)],
            send_sem=send_sem.at[i],
            recv_sem=recv_sem.at[src],
            device_id={"seq": lax.rem(me + i, n)},
            device_id_type=MESH).wait()


def direct(cache_in, page_counts, tail_tokens, assignment):
    n, subs = lax.axis_size("seq"), lax.axis_size("sub")
    pages, layers, piece = cache_in.shape
    vmem = pl.BlockSpec(memory_space=pltpu.VMEM)
    smem = pl.BlockSpec(memory_space=pltpu.SMEM)
    return pl.pallas_call(
        functools.partial(exchange, n, subs),
        out_shape=(jax.ShapeDtypeStruct((MAXP, layers, piece * n), cache_in.dtype),
                   jax.ShapeDtypeStruct((layers, MAXP), jnp.float32)),
        in_specs=[smem, smem, smem, vmem],
        out_specs=(vmem, vmem),
        scratch_shapes=[
            pltpu.VMEM((n, MAXP, layers, piece), cache_in.dtype),
            pltpu.VMEM((piece // LATENT + 1, layers, piece), cache_in.dtype),
            pltpu.VMEM((n, layers, LANES), jnp.float32),
            pltpu.VMEM((n * subs, layers, LANES), jnp.float32),
            pltpu.SemaphoreType.DMA((n,)),
            pltpu.SemaphoreType.DMA((n,)),
            pltpu.SemaphoreType.DMA((n * subs,)),
            pltpu.SemaphoreType.DMA((n * subs,)),
            pltpu.SemaphoreType.DMA,
        ],
        compiler_params=pltpu.CompilerParams(collective_id=0, has_side_effects=True),
    )(page_counts, tail_tokens, assignment, cache_in)


def shards(cache_in, page_counts, tail_tokens, assignment):
    piece = cache_in.shape[2]
    whole_tiles = piece % LANES == 0 and piece % LATENT == 0
    return (direct if whole_tiles else general)(cache_in, page_counts, tail_tokens, assignment)


def solution(mesh):
    placed = (P("groups", None, ("sub", "seq")), P("groups"), P("groups"), P("groups"))
    return jax.shard_map(
        shards,
        mesh=mesh,
        in_specs=placed,
        out_specs=(P(("groups", "seq"), None, "sub"), P(None, ("groups", "seq"))),
        check_vma=False,
    )
```

```python
import functools

import jax
import jax.numpy as jnp
from jax import lax
from jax.experimental import pallas as pl
from jax.experimental.pallas import tpu as pltpu
from jax.sharding import PartitionSpec as P

LATENT = 576
PAGE = 64
MAXP = 8
LANES = 128
ROW_CHIPS = 2
MESH = pl.DeviceIdType.MESH


def by_device(matches, values):
    return jnp.sum(jnp.where(matches, values[None, :], 0), axis=1)


def general(cache_in, page_counts, tail_tokens, assignment):
    seq_count = lax.axis_size("seq")
    own_index = lax.axis_index("seq")
    sub_index = lax.axis_index("sub")
    total_pages, layer_count, piece = cache_in.shape
    starts = jnp.cumsum(page_counts) - page_counts
    device_ids = jnp.arange(seq_count, dtype=jnp.int32)
    matches = assignment[None, :] == device_ids[:, None]
    dest_counts = by_device(matches, page_counts)
    dest_starts = by_device(matches, starts)
    dest_tails = by_device(matches, tail_tokens)
    slot_ids = jnp.arange(seq_count * MAXP, dtype=jnp.int32)
    page_rank = slot_ids % MAXP
    counts_at = jnp.repeat(dest_counts, MAXP)
    starts_at = jnp.repeat(dest_starts, MAXP)
    tails_at = jnp.repeat(dest_tails, MAXP)
    in_use = page_rank < counts_at
    source_rows = jnp.where(in_use, starts_at + page_rank, 0)
    filled = jnp.where(in_use, jnp.where(page_rank < counts_at - 1, PAGE, tails_at), 0)
    column = (sub_index * seq_count + own_index) * piece + jnp.arange(piece, dtype=jnp.int32)
    token_of = column // LATENT
    kept_mask = token_of[None, :] < filled[:, None]
    zero_value = jnp.zeros((), cache_in.dtype)
    fetched = jnp.take(cache_in, source_rows, axis=0)
    packed = jnp.where(kept_mask[:, None, :], fetched, zero_value)
    cache_out = lax.all_to_all(packed, "seq", split_axis=0, concat_axis=2, tiled=True)
    squares = jnp.sum(jnp.square(cache_out.astype(jnp.float32)), axis=2)
    squares = lax.psum(squares, "sub")
    checksum = jnp.sqrt(1.0 + squares / (PAGE * LATENT)).T
    return (cache_out, checksum)


def exchange(n, subs, counts_in, tails_in, assign_in, x_in, out, chk, send, tab, part, parts_in,
             send_sem, recv_sem, psend_sem, precv_sem, ready_sem, own_sem, in_sem,
             x, counts, tails, assign):
    me = lax.axis_index("seq")
    sub = lax.axis_index("sub")
    pages, layers, piece = x.shape
    tokens = piece // LATENT
    own_id = me * subs + sub
    line = n // ROW_CHIPS
    z, col = me // ROW_CHIPS, me % ROW_CHIPS
    steps = [(dz, dx) for dx in range(ROW_CHIPS) for dz in range(1 - line, line) if dz or dx]
    steps.sort(key=lambda step: (-abs(step[0]), -step[1]))

    def inside(step):
        return jnp.logical_and(z + step[0] >= 0, z + step[0] < line)

    def peer(step):
        return (z + step[0]) * ROW_CHIPS + (col + step[1]) % ROW_CHIPS

    def device(other):
        return {"seq": other // subs, "sub": other % subs}

    everyone = range(n * subs)
    arrivals = [pltpu.make_async_copy(a, b, in_sem.at[k]) for k, (a, b) in enumerate(
        ((counts_in, counts), (tails_in, tails), (assign_in, assign), (x_in, x)))]
    for copy in arrivals:
        copy.start()
    barrier = pltpu.get_barrier_semaphore()
    for other in everyone:
        @pl.when(other > own_id)
        def _():
            pl.semaphore_signal(
                barrier, inc=1, device_id=device(other), device_id_type=MESH)

    column = lax.broadcasted_iota(jnp.int32, (layers, piece), 1)
    for f in range(tokens + 1):
        tab[f] = jnp.where(column < f * LATENT, 1.0, 0.0).astype(x.dtype)

    for copy in arrivals:
        copy.wait()
    reqs = counts.shape[0]
    packed, begin = [], jnp.int32(0)
    for r in range(reqs):
        packed.append((begin * 16 + counts[r]) * 128 + tails[r])
        begin = begin + counts[r]
    base = (sub * n + me) * tokens

    for dest in range(n):
        info = jnp.int32(0)
        for r in range(reqs):
            info = info + jnp.where(assign[r] == dest, packed[r], 0)
        tail = info & 127
        count = (info >> 7) & 15
        start = info >> 11
        for k in range(MAXP):
            used = k < count
            row = jnp.where(used, start + k, 0)
            filled = jnp.where(used, jnp.where(k < count - 1, PAGE, tail), 0)
            keep = jnp.clip(filled - base, 0, tokens)
            send[dest, k] = x[row] * tab[keep]

    def columns(source):
        return out.at[:, :, pl.ds(pl.multiple_of(source * piece, LANES), piece)]

    def piece_copy(dest, source):
        return pltpu.make_async_remote_copy(
            src_ref=send.at[dest],
            dst_ref=columns(source),
            send_sem=send_sem.at[dest],
            recv_sem=recv_sem.at[source],
            device_id={"seq": dest},
            device_id_type=MESH)

    def part_copy(i, j, source):
        dest = (me + i) % n
        return pltpu.make_async_remote_copy(
            src_ref=part.at[dest],
            dst_ref=parts_in.at[source],
            send_sem=psend_sem.at[i * subs + j],
            recv_sem=precv_sem.at[source],
            device_id={"seq": dest, "sub": (sub + j) % subs},
            device_id_type=MESH)

    own_copy = pltpu.make_async_copy(send.at[me], columns(me), own_sem)

    @pl.when(own_id > 0)
    def _():
        pl.semaphore_wait(barrier, own_id)

    for other in everyone:
        @pl.when(other < own_id)
        def _():
            pl.semaphore_signal(
                ready_sem.at[own_id], inc=1, device_id=device(other), device_id_type=MESH)
    for step in steps:
        @pl.when(jnp.logical_and(inside(step), peer(step) < me))
        def _():
            piece_copy(peer(step), me).start()
    own_copy.start()
    for dest in range(1, n):
        @pl.when(dest > me)
        def _():
            pl.semaphore_wait(ready_sem.at[dest * subs + sub], 1)
            piece_copy(dest, me).start()

    lane = lax.broadcasted_iota(jnp.int32, (layers, LANES), 1)
    for dest in range(n):
        total = jnp.zeros((layers, LANES), jnp.float32)
        for k in range(MAXP):
            v = send[dest, k].astype(jnp.float32)
            s = jnp.sum(v * v, axis=1, keepdims=True)
            total = jnp.where(lane == k, s, total)
        part[dest] = total
    parts_in[own_id] = part[me]
    for other in everyone:
        @pl.when(jnp.logical_and(other > own_id, other % subs != sub))
        def _():
            pl.semaphore_wait(ready_sem.at[other], 1)
    others = [(i, j) for i in range(n) for j in range(subs) if i or j]
    for i, j in others:
        part_copy(i, j, own_id).start()

    own_copy.wait()
    for i in range(1, n):
        pltpu.make_async_remote_copy(
            src_ref=send.at[(me + i) % n],
            dst_ref=columns((me + n - i) % n),
            send_sem=send_sem.at[(me + i) % n],
            recv_sem=recv_sem.at[(me + n - i) % n],
            device_id={"seq": (me + i) % n},
            device_id_type=MESH).wait()
    for i, j in others:
        part_copy(i, j, (me + n - i) % n * subs + (sub + subs - j) % subs).wait()
    total = jnp.sum(parts_in[...], axis=0)
    chk[...] = jnp.sqrt(1.0 + total / (PAGE * LATENT))[:, :MAXP]


def direct(cache_in, page_counts, tail_tokens, assignment):
    n, subs = lax.axis_size("seq"), lax.axis_size("sub")
    pages, layers, piece = cache_in.shape
    vmem = pl.BlockSpec(memory_space=pltpu.VMEM)
    return pl.pallas_call(
        functools.partial(exchange, n, subs),
        out_shape=(pltpu.VMEM((MAXP, layers, piece * n), cache_in.dtype),
                   pltpu.VMEM((layers, MAXP), jnp.float32)),
        in_specs=[pl.BlockSpec(memory_space=pl.ANY)] * 4,
        out_specs=(vmem, vmem),
        scratch_shapes=[
            pltpu.VMEM((n, MAXP, layers, piece), cache_in.dtype),
            pltpu.VMEM((piece // LATENT + 1, layers, piece), cache_in.dtype),
            pltpu.VMEM((n, layers, LANES), jnp.float32),
            pltpu.VMEM((n * subs, layers, LANES), jnp.float32),
            pltpu.SemaphoreType.DMA((n,)),
            pltpu.SemaphoreType.DMA((n,)),
            pltpu.SemaphoreType.DMA((n * subs,)),
            pltpu.SemaphoreType.DMA((n * subs,)),
            pltpu.SemaphoreType.REGULAR((n * subs,)),
            pltpu.SemaphoreType.DMA,
            pltpu.SemaphoreType.DMA((4,)),
            pltpu.VMEM(cache_in.shape, cache_in.dtype),
            pltpu.SMEM(page_counts.shape, jnp.int32),
            pltpu.SMEM(page_counts.shape, jnp.int32),
            pltpu.SMEM(page_counts.shape, jnp.int32),
        ],
        compiler_params=pltpu.CompilerParams(collective_id=0, has_side_effects=True),
    )(page_counts, tail_tokens, assignment, cache_in)


def shards(cache_in, page_counts, tail_tokens, assignment):
    piece = cache_in.shape[2]
    whole_tiles = piece % LANES == 0 and piece % LATENT == 0 and lax.axis_size("seq") % ROW_CHIPS == 0
    return (direct if whole_tiles else general)(cache_in, page_counts, tail_tokens, assignment)


def solution(mesh):
    placed = (P("groups", None, ("sub", "seq")), P("groups"), P("groups"), P("groups"))
    return jax.shard_map(
        shards,
        mesh=mesh,
        in_specs=placed,
        out_specs=(P(("groups", "seq"), None, "sub"), P(None, ("groups", "seq"))),
        check_vma=False,
    )
```

```python
import functools

import jax
import jax.numpy as jnp
from jax import lax
from jax.experimental import pallas as pl
from jax.experimental.pallas import tpu as pltpu
from jax.sharding import PartitionSpec as P

LATENT = 576
PAGE = 64
MAXP = 8
LANES = 128
ROW_CHIPS = 2
MESH = pl.DeviceIdType.MESH


def by_device(matches, values):
    return jnp.sum(jnp.where(matches, values[None, :], 0), axis=1)


def general(cache_in, page_counts, tail_tokens, assignment):
    seq_count = lax.axis_size("seq")
    own_index = lax.axis_index("seq")
    sub_index = lax.axis_index("sub")
    total_pages, layer_count, piece = cache_in.shape
    starts = jnp.cumsum(page_counts) - page_counts
    device_ids = jnp.arange(seq_count, dtype=jnp.int32)
    matches = assignment[None, :] == device_ids[:, None]
    dest_counts = by_device(matches, page_counts)
    dest_starts = by_device(matches, starts)
    dest_tails = by_device(matches, tail_tokens)
    slot_ids = jnp.arange(seq_count * MAXP, dtype=jnp.int32)
    page_rank = slot_ids % MAXP
    counts_at = jnp.repeat(dest_counts, MAXP)
    starts_at = jnp.repeat(dest_starts, MAXP)
    tails_at = jnp.repeat(dest_tails, MAXP)
    in_use = page_rank < counts_at
    source_rows = jnp.where(in_use, starts_at + page_rank, 0)
    filled = jnp.where(in_use, jnp.where(page_rank < counts_at - 1, PAGE, tails_at), 0)
    column = (sub_index * seq_count + own_index) * piece + jnp.arange(piece, dtype=jnp.int32)
    token_of = column // LATENT
    kept_mask = token_of[None, :] < filled[:, None]
    zero_value = jnp.zeros((), cache_in.dtype)
    fetched = jnp.take(cache_in, source_rows, axis=0)
    packed = jnp.where(kept_mask[:, None, :], fetched, zero_value)
    cache_out = lax.all_to_all(packed, "seq", split_axis=0, concat_axis=2, tiled=True)
    squares = jnp.sum(jnp.square(cache_out.astype(jnp.float32)), axis=2)
    squares = lax.psum(squares, "sub")
    checksum = jnp.sqrt(1.0 + squares / (PAGE * LATENT)).T
    return (cache_out, checksum)


def exchange(n, subs, counts_in, tails_in, assign_in, x_in, out, chk, send, tab, part, parts_in,
             send_sem, recv_sem, psend_sem, precv_sem, ready_sem, own_sem, in_sem,
             x, counts, tails, assign):
    me = lax.axis_index("seq")
    sub = lax.axis_index("sub")
    pages, layers, piece = x.shape
    tokens = piece // LATENT
    own_id = me * subs + sub
    line = n // ROW_CHIPS
    z, col = me // ROW_CHIPS, me % ROW_CHIPS
    steps = [(dz, dx) for dx in range(ROW_CHIPS) for dz in range(1 - line, line) if dz or dx]
    steps.sort(key=lambda step: (-abs(step[0]), -step[1]))

    def inside(step):
        return jnp.logical_and(z + step[0] >= 0, z + step[0] < line)

    def peer(step):
        return (z + step[0]) * ROW_CHIPS + (col + step[1]) % ROW_CHIPS

    def device(other):
        return {"seq": other // subs, "sub": other % subs}

    everyone = range(n * subs)
    arrivals = [pltpu.make_async_copy(a, b, in_sem.at[k]) for k, (a, b) in enumerate(
        ((counts_in, counts), (tails_in, tails), (assign_in, assign), (x_in, x)))]
    for copy in arrivals:
        copy.start()
    barrier = pltpu.get_barrier_semaphore()
    for other in everyone:
        @pl.when(other > own_id)
        def _():
            pl.semaphore_signal(
                barrier, inc=1, device_id=device(other), device_id_type=MESH)

    column = lax.broadcasted_iota(jnp.int32, (layers, piece), 1)
    for f in range(tokens + 1):
        tab[f] = jnp.where(column < f * LATENT, 1.0, 0.0).astype(x.dtype)

    for copy in arrivals:
        copy.wait()
    reqs = counts.shape[0]
    packed, begin = [], jnp.int32(0)
    for r in range(reqs):
        packed.append((begin * 16 + counts[r]) * 128 + tails[r])
        begin = begin + counts[r]
    base = (sub * n + me) * tokens

    for dest in range(n):
        info = jnp.int32(0)
        for r in range(reqs):
            info = info + jnp.where(assign[r] == dest, packed[r], 0)
        tail = info & 127
        count = (info >> 7) & 15
        start = info >> 11
        for k in range(MAXP):
            used = k < count
            row = jnp.where(used, start + k, 0)
            filled = jnp.where(used, jnp.where(k < count - 1, PAGE, tail), 0)
            keep = jnp.clip(filled - base, 0, tokens)
            send[dest, k] = x[row] * tab[keep]

    def columns(source):
        return out.at[:, :, pl.ds(pl.multiple_of(source * piece, LANES), piece)]

    def piece_copy(dest, source):
        return pltpu.make_async_remote_copy(
            src_ref=send.at[dest],
            dst_ref=columns(source),
            send_sem=send_sem.at[dest],
            recv_sem=recv_sem.at[source],
            device_id={"seq": dest},
            device_id_type=MESH)

    def part_copy(i, j, source):
        dest = (me + i) % n
        return pltpu.make_async_remote_copy(
            src_ref=part.at[dest],
            dst_ref=parts_in.at[source],
            send_sem=psend_sem.at[i * subs + j],
            recv_sem=precv_sem.at[source],
            device_id={"seq": dest, "sub": (sub + j) % subs},
            device_id_type=MESH)

    own_copy = pltpu.make_async_copy(send.at[me], columns(me), own_sem)

    @pl.when(own_id > 0)
    def _():
        pl.semaphore_wait(barrier, own_id)

    for other in everyone:
        @pl.when(other < own_id)
        def _():
            pl.semaphore_signal(
                ready_sem.at[own_id], inc=1, device_id=device(other), device_id_type=MESH)
    for step in steps:
        @pl.when(jnp.logical_and(inside(step), peer(step) < me))
        def _():
            piece_copy(peer(step), me).start()
    own_copy.start()
    for dest in range(1, n):
        @pl.when(dest > me)
        def _():
            pl.semaphore_wait(ready_sem.at[dest * subs + sub], 1)
            piece_copy(dest, me).start()

    lane = lax.broadcasted_iota(jnp.int32, (layers, LANES), 1)
    for dest in range(n):
        total = jnp.zeros((layers, LANES), jnp.float32)
        for k in range(MAXP):
            v = send[dest, k].astype(jnp.float32)
            s = jnp.sum(v * v, axis=1, keepdims=True)
            total = jnp.where(lane == k, s, total)
        part[dest] = total
    parts_in[own_id] = part[me]
    for other in everyone:
        @pl.when(jnp.logical_and(other > own_id, other % subs != sub))
        def _():
            pl.semaphore_wait(ready_sem.at[other], 1)
    others = [(i, j) for i in range(n) for j in range(subs) if i or j]
    for i, j in others:
        part_copy(i, j, own_id).start()

    own_copy.wait()
    for i in range(1, n):
        pltpu.make_async_remote_copy(
            src_ref=send.at[(me + i) % n],
            dst_ref=columns((me + n - i) % n),
            send_sem=send_sem.at[(me + i) % n],
            recv_sem=recv_sem.at[(me + n - i) % n],
            device_id={"seq": (me + i) % n},
            device_id_type=MESH).wait()
    for i, j in others:
        part_copy(i, j, (me + n - i) % n * subs + (sub + subs - j) % subs).wait()
    total = jnp.sum(parts_in[...], axis=0)
    chk[...] = jnp.sqrt(1.0 + total / (PAGE * LATENT))[:, :MAXP]


def place(pages_in, sums_in, pages, sums, sem):
    copies = [pltpu.make_async_copy(a, b, sem.at[k]) for k, (a, b) in enumerate(
        ((pages_in, pages), (sums_in, sums)))]
    for copy in copies:
        copy.start()
    for copy in copies:
        copy.wait()


def direct(cache_in, page_counts, tail_tokens, assignment):
    n, subs = lax.axis_size("seq"), lax.axis_size("sub")
    pages, layers, piece = cache_in.shape
    vmem = pl.BlockSpec(memory_space=pltpu.VMEM)
    landed = pl.pallas_call(
        functools.partial(exchange, n, subs),
        out_shape=(pltpu.VMEM((MAXP, layers, piece * n), cache_in.dtype),
                   pltpu.VMEM((layers, MAXP), jnp.float32)),
        in_specs=[pl.BlockSpec(memory_space=pl.ANY)] * 4,
        out_specs=(vmem, vmem),
        scratch_shapes=[
            pltpu.VMEM((n, MAXP, layers, piece), cache_in.dtype),
            pltpu.VMEM((piece // LATENT + 1, layers, piece), cache_in.dtype),
            pltpu.VMEM((n, layers, LANES), jnp.float32),
            pltpu.VMEM((n * subs, layers, LANES), jnp.float32),
            pltpu.SemaphoreType.DMA((n,)),
            pltpu.SemaphoreType.DMA((n,)),
            pltpu.SemaphoreType.DMA((n * subs,)),
            pltpu.SemaphoreType.DMA((n * subs,)),
            pltpu.SemaphoreType.REGULAR((n * subs,)),
            pltpu.SemaphoreType.DMA,
            pltpu.SemaphoreType.DMA((4,)),
            pltpu.VMEM(cache_in.shape, cache_in.dtype),
            pltpu.SMEM(page_counts.shape, jnp.int32),
            pltpu.SMEM(page_counts.shape, jnp.int32),
            pltpu.SMEM(page_counts.shape, jnp.int32),
        ],
        compiler_params=pltpu.CompilerParams(collective_id=0, has_side_effects=True),
    )(page_counts, tail_tokens, assignment, cache_in)
    return pl.pallas_call(
        place,
        out_shape=tuple(jax.ShapeDtypeStruct(a.shape, a.dtype) for a in landed),
        in_specs=[vmem] * 2,
        out_specs=(pl.BlockSpec(memory_space=pltpu.HBM),) * 2,
        scratch_shapes=[pltpu.SemaphoreType.DMA((2,))],
    )(*(pltpu.with_memory_space_constraint(a, pltpu.VMEM) for a in landed))


def shards(cache_in, page_counts, tail_tokens, assignment):
    piece = cache_in.shape[2]
    whole_tiles = piece % LANES == 0 and piece % LATENT == 0 and lax.axis_size("seq") % ROW_CHIPS == 0
    return (direct if whole_tiles else general)(cache_in, page_counts, tail_tokens, assignment)


def solution(mesh):
    placed = (P("groups", None, ("sub", "seq")), P("groups"), P("groups"), P("groups"))
    return jax.shard_map(
        shards,
        mesh=mesh,
        in_specs=placed,
        out_specs=(P(("groups", "seq"), None, "sub"), P(None, ("groups", "seq"))),
        check_vma=False,
    )
```
